128 devices in a mesh: dp: 32 (over x, z_lo, y), expert: 4 (over z_hi, core).
Axes of the slice: x: 4, y: 4, z: 4 (z_hi: 2, z_lo: 2; z = z_hi * 2 + z_lo), core: 2. Of those that a mesh axis runs over, the one named last changes fastest.
Arguments:
- cotangent: bfloat16 [131072, 2048], P(('dp', 'expert')), may hold values from -6 to 6
- route_ids: int32 [131072, 6], P(('dp', 'expert')), may hold values from 0 to 63, all different within a row; in each aligned block of 1024 rows (0 to 1023, 1024 to 2047, ...) at most 192 rows name the same one
- route_weights: float32 [131072, 6], P(('dp', 'expert')), may hold values from 0.02 to 1
- hidden: bfloat16 [8, 24576, 1408], P('expert', 'dp'), may hold values from -6 to 6
- master: float32 [1408, 8, 2048], P('dp', 'expert'), may hold values from -0.3 to 0.3
- first_moment: float32 [1408, 8, 2048], P('dp', 'expert'), may hold values from -1.2 to 1.2
- second_moment: float32 [1408, 8, 2048], P('dp', 'expert'), may hold values from 0.002 to 0.05
Outputs:
- new_master: float32 [1408, 8, 2048], P('dp', 'expert')
- new_first: float32 [1408, 8, 2048], P('dp', 'expert')
- new_second: float32 [1408, 8, 2048], P('dp', 'expert')
The draws below stay inside these ranges and needn't reach their ends.
Inputs may be any that keep to these rules, and one draw needn't show every extreme that they name: `route_ids`: each row names 6 different experts. Within the 1024 rows of one device no expert is named by more than 192 rows.
All inputs are finite; a program needn't handle non-finite values.
Results may differ from the reference program's by a relative error of at most 0.0019.
Values may be sent and summed in bfloat16 or wider, within the bound.
No kernel may reach another device: no remote copies, remote signals or barrier semaphores. Data moves between devices by JAX's collectives and lax.ppermute only.
A program may use at most 128 MiB of HBM per device.

```python
import math
import jax
import jax.numpy as jnp
import numpy as np
from jax import lax

D = 2048
F = 1408
N_ROUTED = 64
TOP = 6
EXP_DEV = 2
TOK_DEV = 1024
CAP = 192
WINDOW = 8
TOKENS = 131072
N_DP = 32
N_EXPERT = 4


def block_scale(own_key, dims, shards, smallest, high):
    def one(dim, blocks):
        draws = jax.random.uniform(jax.random.fold_in(jax.random.fold_in(own_key, 6), dim), (blocks,), jnp.float32, smallest / len(shards), high / len(shards))
        return jnp.repeat(jnp.exp(draws), dims[dim] // blocks).reshape((-1,) + (1,) * (len(dims) - dim - 1))

    factor_of = one(*shards[0])
    for cut in shards[1:]:
        factor_of = factor_of * one(*cut)
    return factor_of


def shared_out(stream_key, own, number, rows, number_of, top, limit, lean):
    sequence = jax.random.permutation(stream_key, number_of)
    packed, usual = load_shares(number_of, rows * top, limit, lean, True), load_shares(number_of, rows * top, limit, lean, False)
    places = jnp.arange(number_of)

    def named(sizes, turn):
        used = int((sizes > 0).sum())
        fixed = max(1, used // 4)
        passed = fixed + (places - fixed + turn * (used - fixed)) % max(1, number_of - fixed)
        return jnp.zeros((number_of,), jnp.int32).at[sequence[jnp.where(places < fixed, places, passed)]].set(jnp.asarray(sizes, jnp.int32))

    sizes = jnp.where(number % 4 == 0, named(packed, number // 4), named(usual, number - number // 4 - 1))
    mixed = jax.random.permutation(jax.random.fold_in(own, 3), number_of)
    donor, sink = mixed[0:number_of // 2 * 2:2], mixed[1:number_of // 2 * 2:2]
    margin = jnp.minimum(sizes[donor] - 1, limit - sizes[sink]) // 2
    margin = jnp.where((donor == sequence[0]) | (sink == sequence[0]) | (sizes[sink] == 0), 0, jnp.maximum(margin, 0))
    passed = jax.random.randint(jax.random.fold_in(own, 4), (number_of // 2,), 0, 1 << 20) % (margin + 1)
    sizes = sizes.at[donor].add(-passed).at[sink].add(passed)
    items = jnp.searchsorted(jnp.cumsum(sizes), jnp.arange(rows * top), side="right").astype(jnp.int32)
    table = items.reshape(top, rows).T
    table = table[jax.random.permutation(jax.random.fold_in(own, 1), rows)]
    turn = jax.random.randint(jax.random.fold_in(own, 2), (rows, 1), 0, top)
    return jnp.take_along_axis(table, (jnp.arange(top)[None, :] + turn) % top, axis=1)


def load_shares(number_of, total, limit, skew, full):
    portions = [(1 << 20) // math.isqrt(standing ** skew) + 1 for standing in range(1, number_of + 1)]
    largest = limit if full else min(limit, max(-(-total // number_of), total * portions[0] // sum(portions)))
    least = 1 if total - largest >= number_of - 1 else 0
    holding, spare = [largest] + [least] * (number_of - 1), total - largest - least * (number_of - 1)
    while spare > 0:
        candidates = [i for i in range(1, number_of) if holding[i] < largest] or [i for i in range(1, number_of) if holding[i] < limit]
        pool, remaining = sum([portions[i] for i in candidates]), spare
        for i in candidates:
            addition = min(limit - holding[i], max(1, remaining * portions[i] // pool), spare)
            holding[i] = holding[i] + addition
            spare = spare - addition
    return np.array(holding)


def bell_draw(rng, shape, width, reach, pieces=(), kind=jnp.bfloat16):
    entries = width * jax.random.normal(rng, shape, jnp.float32)
    if pieces:
        entries = entries * block_scale(rng, shape, pieces, -0.22, 0.18)
    return jnp.clip(entries, -reach, reach).astype(kind)


def setup_inputs(seed: int = 0) -> dict:
    splits = jax.random.split(jax.random.key(seed), 8)
    cotangent = bell_draw(splits[0], (TOKENS, D), 1.0, 6.0, ((0, 128),))
    route_ids_keys = jax.random.split(jax.random.fold_in(splits[1], 1), TOKENS // TOK_DEV)
    route_ids_turns = jax.random.permutation(jax.random.fold_in(splits[1], 3), TOKENS // TOK_DEV)
    route_ids = jax.vmap(lambda own, number: shared_out(jax.random.fold_in(splits[1], 2), own, number, TOK_DEV, N_ROUTED, TOP, CAP, 2))(route_ids_keys, route_ids_turns).reshape((TOKENS, TOP))
    route_weights = jnp.clip(jnp.exp(math.log(1.0) - 3.912023 * jax.random.uniform(splits[2], (TOKENS, TOP), jnp.float32) ** block_scale(splits[2], (TOKENS, TOP), ((0, 128),), -0.2, 0.2)), 0.02, 1.0)
    hidden = bell_draw(splits[3], (WINDOW, N_DP * N_EXPERT * CAP, F), 1.0, 6.0, ((0, 4), (1, 32)))
    master = bell_draw(splits[4], (F, WINDOW, D), 0.05, 0.3, ((0, 32), (1, 4)), jnp.float32)
    first_moment = bell_draw(splits[5], (F, WINDOW, D), 0.2, 1.2, ((0, 32), (1, 4)), jnp.float32)
    second_moment = jnp.clip(jnp.exp(math.log(0.05) - 3.218876 * jax.random.uniform(splits[6], (F, WINDOW, D), jnp.float32) ** block_scale(splits[6], (F, WINDOW, D), ((0, 32), (1, 4)), -0.2, 0.2)), 0.002, 0.05)
    return dict(cotangent=cotangent, route_ids=route_ids, route_weights=route_weights, hidden=hidden, master=master, first_moment=first_moment, second_moment=second_moment)


beta_one = 0.9
beta_two = 0.999
learning_rate = 0.001
epsilon = 1e-08
decay_rate = 0.1
step_count = 4.0

def slot_table(route_ids, route_weights, window, capacity, local_count, groups):
    tokens = route_ids.shape[0]
    onehot = (route_ids[:, :, None] == jnp.arange(window, dtype=jnp.int32)[None, None, :]).astype(jnp.int32)
    counts = lax.optimization_barrier(jnp.sum(onehot, axis=1))
    before = jnp.cumsum(counts, axis=0) - counts
    ranks = lax.optimization_barrier(jnp.sum(onehot * before[:, None, :], axis=2)).astype(jnp.int32)
    inside = route_ids < window
    position = route_ids % local_count * (groups * capacity) + route_ids // local_count * capacity + ranks
    position = jnp.where(inside, position, window * capacity).astype(jnp.int32)
    anchor = jnp.broadcast_to(jnp.arange(tokens, dtype=jnp.int32)[:, None], route_ids.shape)
    slot_anchor = jnp.zeros((window * capacity + 1,), jnp.int32).at[position.reshape(-1)].set(anchor.reshape(-1))
    masked = jnp.where(inside, route_weights, jnp.zeros_like(route_weights))
    slot_weight = jnp.zeros((window * capacity + 1,), route_weights.dtype).at[position.reshape(-1)].set(masked.reshape(-1))
    return (slot_anchor[:-1], slot_weight[:-1])

def reference(cotangent, route_ids, route_weights, hidden, master, first_moment, second_moment):
    blocks = N_DP * N_EXPERT
    cot_blocks = cotangent.reshape(blocks, TOK_DEV, D)
    id_blocks = route_ids.reshape(blocks, TOK_DEV, TOP)
    weight_blocks = route_weights.reshape(blocks, TOK_DEV, TOP)
    block_index = jnp.arange(blocks, dtype=jnp.int32)

    def accumulate(total, inputs):
        cot_block, id_block, weight_block, number = inputs
        slot_anchor, slot_weight = slot_table(id_block, weight_block, WINDOW, CAP, EXP_DEV, N_EXPERT)
        scaled = (cot_block[slot_anchor].astype(jnp.float32) * slot_weight[:, None]).astype(jnp.bfloat16)
        scaled = scaled.reshape(EXP_DEV, N_EXPERT, CAP, D).transpose(1, 0, 2, 3).reshape(WINDOW, CAP, D)
        start = (number * CAP).astype(jnp.int32)
        hidden_block = lax.dynamic_slice_in_dim(hidden, start, CAP, 1)
        total = total + jnp.einsum('kcf,kcd->kfd', hidden_block.astype(jnp.float32), scaled.astype(jnp.float32))
        return (total, None)
    initial = jnp.zeros((WINDOW, F, D), jnp.float32)
    summed, _ = lax.scan(accumulate, initial, (cot_blocks, id_blocks, weight_blocks, block_index))
    gradient = summed.transpose(1, 0, 2) / jnp.sqrt(jnp.float32(N_EXPERT * CAP))
    new_first = beta_one * first_moment + (1.0 - beta_one) * gradient
    new_second = beta_two * second_moment + (1.0 - beta_two) * gradient * gradient
    corrected_first = new_first / (1.0 - beta_one ** step_count)
    corrected_second = new_second / (1.0 - beta_two ** step_count)
    update = corrected_first / (jnp.sqrt(corrected_second) + epsilon) + decay_rate * master
    new_master = master - learning_rate * update
    return (new_master, new_first, new_second)
```

```python
import functools

import jax
import jax.numpy as jnp
from jax import lax
from jax.experimental import pallas as pl
from jax.experimental.pallas import tpu as pltpu
from jax.sharding import PartitionSpec as P

beta_one = 0.9
beta_two = 0.999
learning_rate = 0.001
epsilon = 1e-08
decay_rate = 0.1
step_count = 4.0

CHUNKS = 2
AXES = ("dp", "expert")


def device_of(x, y, z, core):
    return (x % 4 * 8 + z % 2 * 4 + y % 4) * 4 + z // 2 * 2 + core


def moves(step):
    pairs = []
    for x in range(4):
        for y in range(4):
            for z in range(4):
                for core in range(2):
                    pairs.append((device_of(x, y, z, core), device_of(*step(x, y, z, core))))
    return pairs


ALONG_X = {j: moves(lambda x, y, z, core, j=j: (x + j, y, z, core)) for j in (1, 2, 3)}
ALONG_Y = {j: moves(lambda x, y, z, core, j=j: (x, y + j, z, core)) for j in (1, 2, 3)}
PAIR_Z = moves(lambda x, y, z, core: (x, y, z ^ 1, core))
TO_EXPERT = {
    m: moves(lambda x, y, z, core, m=m: (x, y, z ^ (m & 2), core ^ (m & 1))) for m in (1, 2, 3)
}


def send(array, pairs):
    return lax.ppermute(array, AXES, pairs)


def dispatch_body(own_ref, ids_ref, weights_ref, cot_ref, *out_refs):
    capacity = out_refs[0].shape[1]
    tokens = cot_ref.shape[0]
    own = own_ref[0]
    ids = ids_ref[...]
    weights = weights_ref[...]
    cot = cot_ref[...]
    chosen, weight_rows = [], []
    for m in range(4):
        for local in range(2):
            match = ids == 2 * jnp.bitwise_xor(own, m) + local
            chosen.append(jnp.sum(match.astype(jnp.float32), axis=0, keepdims=True))
            weight_rows.append(jnp.sum(jnp.where(match, weights, 0.0), axis=0, keepdims=True))
    taken = jnp.concatenate(chosen, axis=0)
    ahead = lax.broadcasted_iota(jnp.int32, (128, 128), 0) < lax.broadcasted_iota(
        jnp.int32, (128, 128), 1
    )
    ahead = ahead.astype(jnp.float32).astype(jnp.bfloat16)
    offset = jnp.zeros((8, 1), jnp.float32)
    ranks = []
    for start in range(0, tokens, 128):
        tile = taken[:, start : start + 128]
        inside = jnp.dot(tile.astype(jnp.bfloat16), ahead, preferred_element_type=jnp.float32)
        ranks.append(jnp.where(tile > 0.0, inside + offset, -1.0))
        offset = offset + jnp.sum(tile, axis=1, keepdims=True)
    rank = jnp.concatenate(ranks, axis=1).astype(jnp.int32)
    slot = lax.broadcasted_iota(jnp.int32, (capacity, tokens), 0)
    for m in range(4):
        for local in range(2):
            k = 2 * m + local
            mask = rank[k : k + 1, :] == slot
            picked = jnp.dot(
                jnp.where(mask, 1.0, 0.0).astype(jnp.bfloat16),
                cot,
                preferred_element_type=jnp.float32,
            )
            weight = jnp.sum(jnp.where(mask, weight_rows[k], 0.0), axis=1, keepdims=True)
            out_refs[m][local] = (picked * weight).astype(jnp.bfloat16)


def dispatch(own, ids, weights, cotangent, chunk, capacity):
    tokens, width = cotangent.shape
    part = width // CHUNKS
    whole = lambda shape: pl.BlockSpec(shape, lambda i, s: (0,) * len(shape))
    return pl.pallas_call(
        dispatch_body,
        grid_spec=pltpu.PrefetchScalarGridSpec(
            num_scalar_prefetch=1,
            grid=(1,),
            in_specs=[
                whole(ids.shape),
                whole(weights.shape),
                pl.BlockSpec((tokens, part), lambda i, s: (0, chunk)),
            ],
            out_specs=[whole((2, capacity, part))] * 4,
        ),
        out_shape=[jax.ShapeDtypeStruct((2, capacity, part), jnp.bfloat16)] * 4,
        name=f"dispatch_{chunk}",
    )(own, ids, weights, cotangent)


def prepare_body(place_ref, hidden_ref, out_ref):
    local, block = pl.program_id(0), pl.program_id(1)
    rows, hidden_units = out_ref.shape[1], hidden_ref.shape[2]
    share = hidden_units // 32
    capacity = hidden_ref.shape[1] // 4
    x, y, z, own = place_ref[0], place_ref[1], place_ref[2], place_ref[3]
    row = lax.broadcasted_iota(jnp.int32, (rows, 1), 0) + block * rows
    row = row.astype(jnp.float32)
    tile = jnp.floor((row + 0.5) / share)
    rest = row - tile * share
    outer = jnp.floor((tile + 0.5) / 8.0)
    inner = jnp.floor((tile - outer * 8.0 + 0.5) / 2.0)
    last = tile - outer * 8.0 - inner * 2.0
    first = local == 0
    first_base = jnp.where(first, x, y).astype(jnp.float32)
    second_base = jnp.where(first, y, x).astype(jnp.float32)
    outer = outer + first_base
    outer = jnp.where(outer >= 4.0, outer - 4.0, outer)
    inner = inner + second_base
    inner = jnp.where(inner >= 4.0, inner - 4.0, inner)
    last = last + z.astype(jnp.float32)
    last = jnp.where(last >= 2.0, last - 2.0, last)
    outer_stride = jnp.where(first, 8, 1).astype(jnp.float32)
    inner_stride = jnp.where(first, 1, 8).astype(jnp.float32)
    source = (outer * outer_stride + inner * inner_stride + last * 4.0) * share + rest
    unit = lax.broadcasted_iota(jnp.int32, (rows, hidden_units), 1).astype(jnp.float32)
    pick = jnp.where(source == unit, 1.0, 0.0).astype(jnp.bfloat16)
    by_sender = jnp.concatenate(
        [
            hidden_ref[0, pl.ds(jnp.bitwise_xor(own, m) * capacity, capacity), :]
            for m in range(4)
        ],
        axis=0,
    )
    out_ref[0] = lax.dot_general(
        pick, by_sender, (((1,), (1,)), ((), ())), preferred_element_type=jnp.float32
    ).astype(jnp.bfloat16)


def prepare(place, hidden):
    local_count, slots, units = hidden.shape
    return pl.pallas_call(
        prepare_body,
        grid_spec=pltpu.PrefetchScalarGridSpec(
            num_scalar_prefetch=1,
            grid=(local_count, 4),
            in_specs=[pl.BlockSpec((1, slots, units), lambda e, b, s: (e, 0, 0))],
            out_specs=pl.BlockSpec((1, units // 4, slots), lambda e, b, s: (e, b, 0)),
        ),
        out_shape=jax.ShapeDtypeStruct((local_count, units, slots), jnp.bfloat16),
        name="prepare",
    )(place, hidden)


def matmul_body(hidden_ref, r0, r1, r2, r3, *out_refs):
    rows = hidden_ref.shape[1] // 4
    for local in range(2):
        rhs = jnp.concatenate([r[local] for r in (r0, r1, r2, r3)], axis=0)
        for j in range(4):
            product = jnp.dot(
                hidden_ref[local, j * rows : (j + 1) * rows, :],
                rhs,
                preferred_element_type=jnp.float32,
            )
            out = out_refs[4 * local + j]
            out[...] = product.astype(out.dtype)


def partials(hidden, received, chunk):
    part = received[0].shape[2]
    rows = hidden.shape[1] // 4
    kinds = [jnp.float32, jnp.bfloat16, jnp.bfloat16, jnp.bfloat16] * 2
    return pl.pallas_call(
        matmul_body,
        out_shape=[jax.ShapeDtypeStruct((rows, part), kind) for kind in kinds],
        name=f"partials_{chunk}",
    )(hidden, *received)


def gathered_sum(own, sends, along):
    got = [send(block, along[j]) for j, block in zip((1, 2, 3), sends)]
    total = own
    for block in got:
        total = total + block.astype(jnp.float32)
    return total


def quarters(total):
    rows = total.shape[0] // 4
    pieces = [total[j * rows : (j + 1) * rows] for j in range(4)]
    return pieces[0], [piece.astype(jnp.bfloat16) for piece in pieces[1:]]


def shards(cotangent, route_ids, route_weights, hidden, master, first_moment, second_moment):
    groups = lax.axis_size("expert")
    capacity = hidden.shape[1] // groups
    dp = lax.axis_index("dp").astype(jnp.int32)
    own = lax.axis_index("expert").astype(jnp.int32)
    place = jnp.stack([dp // 8, dp % 4, dp // 4 % 2, own])
    ids, weights = route_ids.T, route_weights.T
    turned = None
    gradients = []
    for chunk in range(CHUNKS):
        outgoing = dispatch(own[None], ids, weights, cotangent, chunk, capacity)
        received = [outgoing[0]] + [send(outgoing[m], TO_EXPERT[m]) for m in (1, 2, 3)]
        if turned is None:
            turned = prepare(place, hidden)
        blocks = partials(turned, received, chunk)
        halves = []
        for local, (one, two) in enumerate(((ALONG_X, ALONG_Y), (ALONG_Y, ALONG_X))):
            mine, sends = blocks[4 * local], blocks[4 * local + 1 : 4 * local + 4]
            total = gathered_sum(mine, sends, one)
            mine, sends = quarters(total)
            halves.append(gathered_sum(mine, sends, two))
        both = jnp.stack(halves)
        share = both.shape[1] // 2
        gradients.append(both[:, :share] + send(both[:, share:], PAIR_Z))
    summed = jnp.concatenate(gradients, axis=2).transpose(1, 0, 2)
    gradient = summed / jnp.sqrt(jnp.float32(groups * capacity))
    new_first = beta_one * first_moment + (1.0 - beta_one) * gradient
    new_second = beta_two * second_moment + (1.0 - beta_two) * gradient * gradient
    corrected_first = new_first / (1.0 - beta_one**step_count)
    corrected_second = new_second / (1.0 - beta_two**step_count)
    update = corrected_first / (jnp.sqrt(corrected_second) + epsilon) + decay_rate * master
    new_master = master - learning_rate * update
    return (new_master, new_first, new_second)


def solution(mesh):
    placed = (
        P(("dp", "expert"), None),
        P(("dp", "expert"), None),
        P(("dp", "expert"), None),
        P("expert", "dp", None),
        P("dp", "expert", None),
        P("dp", "expert", None),
        P("dp", "expert", None),
    )
    return jax.shard_map(
        shards,
        mesh=mesh,
        in_specs=placed,
        out_specs=(P("dp", "expert", None), P("dp", "expert", None), P("dp", "expert", None)),
        check_vma=False,
    )
```

```python
import functools

import jax
import jax.numpy as jnp
from jax import lax
from jax.experimental import pallas as pl
from jax.experimental.layout import Layout, with_layout_constraint
from jax.experimental.pallas import tpu as pltpu
from jax.sharding import PartitionSpec as P


beta_one = 0.9
beta_two = 0.999
learning_rate = 0.001
epsilon = 1e-08
decay_rate = 0.1
step_count = 4.0

GROUPS = ((768,), (896, 384))
WAVES = ((0, 1), (2,))
RINGS = (True, True, False)
ROW_MAJOR = Layout(major_to_minor=(0, 1, 2))
WIDE, NARROW = 60 * 1024 * 2**10, 24 * 2**20
AXES = ("dp", "expert")


def device_of(x, y, z, core):
    return (x % 4 * 8 + z % 2 * 4 + y % 4) * 4 + z // 2 * 2 + core


def moves(step):
    pairs = []
    for x in range(4):
        for y in range(4):
            for z in range(4):
                for core in range(2):
                    pairs.append((device_of(x, y, z, core), device_of(*step(x, y, z, core))))
    return pairs


ALONG_X = {j: moves(lambda x, y, z, core, j=j: (x + j, y, z, core)) for j in (1, 2, 3)}
ALONG_Y = {j: moves(lambda x, y, z, core, j=j: (x, y + j, z, core)) for j in (1, 2, 3)}
PAIR_Z = moves(lambda x, y, z, core: (x, y, z ^ 1, core))
TO_EXPERT = {
    m: moves(lambda x, y, z, core, m=m: (x, y, z ^ (m & 2), core ^ (m & 1))) for m in (1, 2, 3)
}


def send(array, pairs):
    return lax.ppermute(array, AXES, pairs)


def dispatch_body(start, own_ref, ids_hbm, weights_hbm, cot_hbm, *refs):
    out_refs, (ids_ref, weights_ref, cot_ref, sems) = refs[:-4], refs[-4:]
    capacity = out_refs[0].shape[1]
    tokens, part = cot_ref.shape
    columns = cot_hbm.at[:, pl.ds(start, part)]
    pairs = ((ids_hbm, ids_ref), (weights_hbm, weights_ref), (columns, cot_ref))
    copies = [pltpu.make_async_copy(a, b, sems.at[n]) for n, (a, b) in enumerate(pairs)]
    for copy in copies:
        copy.start()
    own = own_ref[0]
    copies[0].wait()
    copies[1].wait()
    ids = ids_ref[...]
    weights = weights_ref[...]
    chosen, weight_rows = [], []
    for m in range(4):
        for local in range(2):
            match = ids == 2 * jnp.bitwise_xor(own, m) + local
            chosen.append(jnp.sum(match.astype(jnp.float32), axis=0, keepdims=True))
            weight_rows.append(jnp.sum(jnp.where(match, weights, 0.0), axis=0, keepdims=True))
    taken = jnp.concatenate(chosen, axis=0)
    ahead = lax.broadcasted_iota(jnp.int32, (128, 128), 0) < lax.broadcasted_iota(
        jnp.int32, (128, 128), 1
    )
    ahead = ahead.astype(jnp.float32).astype(jnp.bfloat16)
    offset = jnp.zeros((8, 1), jnp.float32)
    ranks = []
    for start in range(0, tokens, 128):
        tile = taken[:, start : start + 128]
        inside = jnp.dot(tile.astype(jnp.bfloat16), ahead, preferred_element_type=jnp.float32)
        ranks.append(jnp.where(tile > 0.0, inside + offset, -1.0))
        offset = offset + jnp.sum(tile, axis=1, keepdims=True)
    rank = jnp.concatenate(ranks, axis=1).astype(jnp.int32)
    slot = lax.broadcasted_iota(jnp.int32, (capacity, tokens), 0)
    far = (len(out_refs) - 2) // 2
    copies[2].wait()
    for m in (2, 3, 1, 0):
        for local in range(2):
            k = 2 * m + local
            mask = rank[k : k + 1, :] == slot
            picked = jnp.dot(
                jnp.where(mask, 1.0, 0.0).astype(jnp.bfloat16),
                cot_ref[...],
                preferred_element_type=jnp.float32,
            )
            weight = jnp.sum(jnp.where(mask, weight_rows[k], 0.0), axis=1, keepdims=True)
            rows = (picked * weight).astype(jnp.bfloat16)
            if m < 2:
                out_refs[m][local] = rows
            else:
                at = 0
                for out in out_refs[2 + far * (m - 2) : 2 + far * (m - 1)]:
                    out[local] = rows[:, at : at + out.shape[2]]
                    at += out.shape[2]


def dispatch(own, ids, weights, cotangent, widths, start, capacity):
    tokens = cotangent.shape[0]
    part = sum(widths)
    whole = lambda shape: pl.BlockSpec(shape, lambda i, s: (0,) * len(shape))
    shapes = [(2, capacity, part)] * 2 + [(2, capacity, w) for w in widths] * 2
    outs = pl.pallas_call(
        functools.partial(dispatch_body, start),
        grid_spec=pltpu.PrefetchScalarGridSpec(
            num_scalar_prefetch=1,
            grid=(1,),
            in_specs=[pl.BlockSpec(memory_space=pltpu.HBM)] * 3,
            out_specs=[whole(shape) for shape in shapes],
            scratch_shapes=[
                pltpu.VMEM(ids.shape, ids.dtype),
                pltpu.VMEM(weights.shape, weights.dtype),
                pltpu.VMEM((tokens, part), cotangent.dtype),
                pltpu.SemaphoreType.DMA((3,)),
            ],
        ),
        out_shape=[jax.ShapeDtypeStruct(shape, jnp.bfloat16) for shape in shapes],
        compiler_params=pltpu.CompilerParams(vmem_limit_bytes=WIDE if start == 0 else NARROW),
    )(own, ids, weights, cotangent)
    n = len(widths)
    return outs[0], outs[1], outs[2 : 2 + n], outs[2 + n :]


def prepare_body(place_ref, hidden_hbm, out_ref, hidden_ref, sems):
    local, block = pl.program_id(0), pl.program_id(1)

    def copy(n):
        return pltpu.make_async_copy(hidden_hbm.at[n], hidden_ref.at[n], sems.at[n])

    @pl.when((local == 0) & (block == 0))
    def fetch():
        copy(0).start()
        copy(1).start()
        copy(0).wait()

    @pl.when((local == 1) & (block == 0))
    def arrived():
        copy(1).wait()

    rows, hidden_units = out_ref.shape[1], hidden_ref.shape[2]
    share = hidden_units // 32
    capacity = hidden_ref.shape[1] // 4
    x, y, z, own = place_ref[0], place_ref[1], place_ref[2], place_ref[3]
    row = lax.broadcasted_iota(jnp.int32, (rows, 1), 0) + block * rows
    row = row.astype(jnp.float32)
    tile = jnp.floor((row + 0.5) / share)
    rest = row - tile * share
    outer = jnp.floor((tile + 0.5) / 8.0)
    inner = jnp.floor((tile - outer * 8.0 + 0.5) / 2.0)
    last = tile - outer * 8.0 - inner * 2.0
    first = local == 0
    first_base = jnp.where(first, x, y).astype(jnp.float32)
    second_base = jnp.where(first, y, x).astype(jnp.float32)
    outer = outer + first_base
    outer = jnp.where(outer >= 4.0, outer - 4.0, outer)
    inner = inner + second_base
    inner = jnp.where(inner >= 4.0, inner - 4.0, inner)
    last = last + z.astype(jnp.float32)
    last = jnp.where(last >= 2.0, last - 2.0, last)
    outer_stride = jnp.where(first, 8, 1).astype(jnp.float32)
    inner_stride = jnp.where(first, 1, 8).astype(jnp.float32)
    source = (outer * outer_stride + inner * inner_stride + last * 4.0) * share + rest
    unit = lax.broadcasted_iota(jnp.int32, (rows, hidden_units), 1).astype(jnp.float32)
    pick = jnp.where(source == unit, 1.0, 0.0).astype(jnp.bfloat16)
    by_sender = jnp.concatenate(
        [
            hidden_ref[local, pl.ds(jnp.bitwise_xor(own, m) * capacity, capacity), :]
            for m in range(4)
        ],
        axis=0,
    )
    out_ref[0] = lax.dot_general(
        pick, by_sender, (((1,), (1,)), ((), ())), preferred_element_type=jnp.float32
    ).astype(jnp.bfloat16)


def prepare(place, hidden):
    local_count, slots, units = hidden.shape
    return pl.pallas_call(
        prepare_body,
        grid_spec=pltpu.PrefetchScalarGridSpec(
            num_scalar_prefetch=1,
            grid=(local_count, 4),
            in_specs=[pl.BlockSpec(memory_space=pltpu.HBM)],
            out_specs=pl.BlockSpec((1, units // 4, slots), lambda e, b, s: (e, b, 0)),
            scratch_shapes=[
                pltpu.VMEM(hidden.shape, hidden.dtype),
                pltpu.SemaphoreType.DMA((local_count,)),
            ],
        ),
        out_shape=jax.ShapeDtypeStruct((local_count, units, slots), jnp.bfloat16),
        compiler_params=pltpu.CompilerParams(vmem_limit_bytes=20 * 2**20),
        name="prepare",
    )(place, hidden)


def matmul_body(ring, hidden_ref, r0, r1, r2, r3, *out_refs):
    rhs = jnp.concatenate([r[0] for r in (r0, r1, r2, r3)], axis=0)
    product = jnp.dot(hidden_ref[0], rhs, preferred_element_type=jnp.float32)
    half = product.shape[0] // 2
    each = len(out_refs) // 2
    for local in range(2):
        outs = out_refs[each * local : each * (local + 1)]
        for j in range(4):

            @pl.when(pl.program_id(0) == 4 * local + j)
            def store(j=j, outs=outs):
                if ring and j == 2:
                    outs[3][...] = product[:half].astype(jnp.bfloat16)
                    outs[4][...] = product[half:].astype(jnp.bfloat16)
                else:
                    out = outs[2 if ring and j == 3 else j]
                    out[...] = product.astype(out.dtype)


def partials(hidden, near, far, offset, ring):
    capacity, part = far[0].shape[1:]
    rows, slots = hidden.shape[1] // 4, hidden.shape[2]
    wide = jax.ShapeDtypeStruct((rows, part), jnp.float32)
    if ring:
        shapes = [wide] * 3 + [jax.ShapeDtypeStruct((rows // 2, part), jnp.bfloat16)] * 2
    else:
        shapes = [wide] + [jax.ShapeDtypeStruct((rows, part), jnp.bfloat16)] * 3
    near_spec = pl.BlockSpec(
        (pl.Element(1), pl.Element(capacity), pl.Element(part)), lambda i: (i // 4, 0, offset)
    )
    far_spec = pl.BlockSpec((1, capacity, part), lambda i: (i // 4, 0, 0))
    outs = pl.pallas_call(
        functools.partial(matmul_body, ring),
        grid=(8,),
        in_specs=[
            pl.BlockSpec((1, rows, slots), lambda i: (i // 4, i % 4, 0)),
            near_spec,
            near_spec,
            far_spec,
            far_spec,
        ],
        out_specs=[pl.BlockSpec(s.shape, lambda i: (0, 0)) for s in shapes * 2],
        out_shape=shapes * 2,
        compiler_params=pltpu.CompilerParams(vmem_limit_bytes=NARROW),
    )(hidden, *near, *far)
    return outs[: len(shapes)], outs[len(shapes) :]


def to_half(total):
    return (total * 0.03125).astype(jnp.float16)


def from_half(block):
    return block.astype(jnp.float32) * 32.0


def ring_sum(own, ahead, behind, low, high, along):
    half = low.shape[0]
    high = send(high, along[1])
    low = send(low, along[3])
    ahead = jnp.concatenate([ahead[:half], ahead[half:] + high.astype(jnp.float32)])
    behind = jnp.concatenate([behind[:half] + low.astype(jnp.float32), behind[half:]])
    ahead, behind = to_half(ahead), to_half(behind)
    ahead = send(ahead, along[1])
    behind = send(behind, along[3])
    return own + from_half(ahead) + from_half(behind)


def quarters(total):
    rows = total.shape[0] // 4
    pieces = [total[j * rows : (j + 1) * rows] for j in range(4)]
    return pieces[0], [to_half(piece) for piece in pieces[1:]]


def direct_sum(own, sends, along):
    got = []
    for j, block in zip((1, 2, 3), sends):
        got.append(send(block, along[j]))
    for block in got:
        own = own + (from_half(block) if block.dtype == jnp.float16 else block.astype(jnp.float32))
    return own


def step(cotangent, route_ids, route_weights, hidden, master, first_moment, second_moment):
    groups = lax.axis_size("expert")
    capacity = hidden.shape[1] // groups
    dp = lax.axis_index("dp").astype(jnp.int32)
    own = lax.axis_index("expert").astype(jnp.int32)
    place = jnp.stack([dp // 8, dp % 4, dp // 4 % 2, own])
    ids, weights = route_ids.T, route_weights.T
    gradients, received = [], []
    start, turned = 0, None
    for group, widths in enumerate(GROUPS):
        if group == 1:
            place, _ = lax.optimization_barrier((place, received[0][1][0]))
            turned = prepare(place, hidden)
            own, turned = lax.optimization_barrier((own, turned))
        mine, partner, far, farther = dispatch(
            own[None], ids, weights, cotangent, widths, start, capacity
        )
        near = (mine, send(partner, TO_EXPERT[1]))
        offset = 0
        for index, width in enumerate(widths):
            one = send(far[index], TO_EXPERT[2])
            two = send(farther[index], TO_EXPERT[3])
            received.append((near, (mine, one, two), offset))
            offset += width
        start += sum(widths)
    totals = ([], [])
    for chunk, (near, (_, *far), offset) in enumerate(received):
        blocks = partials(turned, near, far, offset, RINGS[chunk])
        for local, along in enumerate((ALONG_X, ALONG_Y)):
            (own_block, *sends) = blocks[local]
            if RINGS[chunk]:
                total = ring_sum(own_block, *sends, along)
            else:
                total = direct_sum(own_block, sends, along)
            totals[local].append(total)
    for members in WAVES:
        halves = []
        for local, along in enumerate((ALONG_Y, ALONG_X)):
            total = jnp.concatenate([totals[local][c] for c in members], axis=1)
            own_block, sends = quarters(total)
            halves.append(direct_sum(own_block, sends, along))
        share = halves[0].shape[0] // 2
        away = jnp.stack([to_half(part[share:]) for part in halves])
        other = send(away, PAIR_Z)
        both = jnp.stack([part[:share] for part in halves]) + from_half(other)
        gradients.append(with_layout_constraint(both.transpose(1, 0, 2), ROW_MAJOR))
    summed = jnp.concatenate(gradients, axis=2)
    gradient = summed / jnp.sqrt(jnp.float32(groups * capacity))
    new_first = beta_one * first_moment + (1.0 - beta_one) * gradient
    new_second = beta_two * second_moment + (1.0 - beta_two) * gradient * gradient
    corrected_first = new_first / (1.0 - beta_one**step_count)
    corrected_second = new_second / (1.0 - beta_two**step_count)
    update = corrected_first / (jnp.sqrt(corrected_second) + epsilon) + decay_rate * master
    new_master = master - learning_rate * update
    return (new_master, new_first, new_second)


def solution(mesh):
    placed = (
        P(("dp", "expert"), None),
        P(("dp", "expert"), None),
        P(("dp", "expert"), None),
        P("expert", "dp", None),
        P("dp", "expert", None),
        P("dp", "expert", None),
        P("dp", "expert", None),
    )
    return jax.shard_map(
        step,
        mesh=mesh,
        in_specs=placed,
        out_specs=(P("dp", "expert", None), P("dp", "expert", None), P("dp", "expert", None)),
        check_vma=False,
    )
```

```python
import functools

import jax
import jax.numpy as jnp
from jax import lax
from jax.experimental import pallas as pl
from jax.experimental.layout import Layout, with_layout_constraint
from jax.experimental.pallas import tpu as pltpu
from jax.sharding import PartitionSpec as P


beta_one = 0.9
beta_two = 0.999
learning_rate = 0.001
epsilon = 1e-08
decay_rate = 0.1
step_count = 4.0

GROUPS = ((768,), (768, 512))
WAVES = ((0, 1), (2,))
RINGS = (False, True, False)
ROW_MAJOR = Layout(major_to_minor=(0, 1, 2))
WIDE, NARROW = 60 * 1024 * 2**10, 24 * 2**20
AXES = ("dp", "expert")


def device_of(x, y, z, core):
    return (x % 4 * 8 + z % 2 * 4 + y % 4) * 4 + z // 2 * 2 + core


def moves(step):
    pairs = []
    for x in range(4):
        for y in range(4):
            for z in range(4):
                for core in range(2):
                    pairs.append((device_of(x, y, z, core), device_of(*step(x, y, z, core))))
    return pairs


ALONG_X = {j: moves(lambda x, y, z, core, j=j: (x + j, y, z, core)) for j in (1, 2, 3)}
ALONG_Y = {j: moves(lambda x, y, z, core, j=j: (x, y + j, z, core)) for j in (1, 2, 3)}
PAIR_Z = moves(lambda x, y, z, core: (x, y, z ^ 1, core))
TO_EXPERT = {
    m: moves(lambda x, y, z, core, m=m: (x, y, z ^ (m & 2), core ^ (m & 1))) for m in (1, 2, 3)
}


def send(array, pairs):
    return lax.ppermute(array, AXES, pairs)


def dispatch_body(start, near, own_ref, ids_hbm, weights_hbm, cot_hbm, *refs):
    out_refs, (ids_ref, weights_ref, cot_ref, sems) = refs[:-4], refs[-4:]
    capacity = out_refs[0].shape[1]
    tokens, part = cot_ref.shape
    columns = cot_hbm.at[:, pl.ds(0, part)]
    pairs = ((ids_hbm, ids_ref), (weights_hbm, weights_ref), (columns, cot_ref))
    copies = [pltpu.make_async_copy(a, b, sems.at[n]) for n, (a, b) in enumerate(pairs)]
    for copy in copies:
        copy.start()
    own = own_ref[0]
    copies[0].wait()
    copies[1].wait()
    ids = ids_ref[...]
    weights = weights_ref[...]
    chosen, weight_rows = [], []
    for m in range(4):
        for local in range(2):
            match = ids == 2 * jnp.bitwise_xor(own, m) + local
            chosen.append(jnp.sum(match.astype(jnp.float32), axis=0, keepdims=True))
            weight_rows.append(jnp.sum(jnp.where(match, weights, 0.0), axis=0, keepdims=True))
    taken = jnp.concatenate(chosen, axis=0)
    ahead = lax.broadcasted_iota(jnp.int32, (128, 128), 0) < lax.broadcasted_iota(
        jnp.int32, (128, 128), 1
    )
    ahead = ahead.astype(jnp.float32).astype(jnp.bfloat16)
    offset = jnp.zeros((8, 1), jnp.float32)
    ranks = []
    for first in range(0, tokens, 128):
        tile = taken[:, first : first + 128]
        inside = jnp.dot(tile.astype(jnp.bfloat16), ahead, preferred_element_type=jnp.float32)
        ranks.append(jnp.where(tile > 0.0, inside + offset, -1.0))
        offset = offset + jnp.sum(tile, axis=1, keepdims=True)
    rank = jnp.concatenate(ranks, axis=1).astype(jnp.int32)
    slot = lax.broadcasted_iota(jnp.int32, (capacity, tokens), 0)
    far_refs = out_refs[2:] if near else out_refs
    far = len(far_refs) // 2
    copies[2].wait()
    for m in (2, 3, 1, 0) if near else (2, 3):
        for local in range(2):
            k = 2 * m + local
            mask = rank[k : k + 1, :] == slot
            picked = jnp.dot(
                jnp.where(mask, 1.0, 0.0).astype(jnp.bfloat16),
                cot_ref[...] if m < 2 else cot_ref[:, start:],
                preferred_element_type=jnp.float32,
            )
            weight = jnp.sum(jnp.where(mask, weight_rows[k], 0.0), axis=1, keepdims=True)
            rows = (picked * weight).astype(jnp.bfloat16)
            if m < 2:
                out_refs[m][local] = rows
            else:
                at = 0
                for out in far_refs[far * (m - 2) : far * (m - 1)]:
                    out[local] = rows[:, at : at + out.shape[2]]
                    at += out.shape[2]


def dispatch(own, ids, weights, cotangent, widths, start, near, capacity):
    part = start + sum(widths)
    whole = lambda shape: pl.BlockSpec(shape, lambda i, s: (0,) * len(shape))
    shapes = [(2, capacity, part)] * 2 if near else []
    shapes = shapes + [(2, capacity, w) for w in widths] * 2
    outs = pl.pallas_call(
        functools.partial(dispatch_body, start, near),
        grid_spec=pltpu.PrefetchScalarGridSpec(
            num_scalar_prefetch=1,
            grid=(1,),
            in_specs=[pl.BlockSpec(memory_space=pltpu.HBM)] * 3,
            out_specs=[whole(shape) for shape in shapes],
            scratch_shapes=[
                pltpu.VMEM(ids.shape, ids.dtype),
                pltpu.VMEM(weights.shape, weights.dtype),
                pltpu.VMEM((cotangent.shape[0], part), cotangent.dtype),
                pltpu.SemaphoreType.DMA((3,)),
            ],
        ),
        out_shape=[jax.ShapeDtypeStruct(shape, jnp.bfloat16) for shape in shapes],
        compiler_params=pltpu.CompilerParams(vmem_limit_bytes=NARROW if near else WIDE),
    )(own, ids, weights, cotangent)
    near_rows, outs = (outs[:2], outs[2:]) if near else (None, outs)
    n = len(widths)
    return near_rows, outs[:n], outs[n:]


def prepare_body(place_ref, hidden_hbm, out_ref, hidden_ref, sems):
    local, block = pl.program_id(0), pl.program_id(1)

    def copy(n):
        return pltpu.make_async_copy(hidden_hbm.at[n], hidden_ref.at[n], sems.at[n])

    @pl.when((local == 0) & (block == 0))
    def fetch():
        copy(0).start()
        copy(1).start()
        copy(0).wait()

    @pl.when((local == 1) & (block == 0))
    def arrived():
        copy(1).wait()

    rows, hidden_units = out_ref.shape[1], hidden_ref.shape[2]
    share = hidden_units // 32
    capacity = hidden_ref.shape[1] // 4
    x, y, z, own = place_ref[0], place_ref[1], place_ref[2], place_ref[3]
    row = lax.broadcasted_iota(jnp.int32, (rows, 1), 0) + block * rows
    row = row.astype(jnp.float32)
    tile = jnp.floor((row + 0.5) / share)
    rest = row - tile * share
    outer = jnp.floor((tile + 0.5) / 8.0)
    inner = jnp.floor((tile - outer * 8.0 + 0.5) / 2.0)
    last = tile - outer * 8.0 - inner * 2.0
    first = local == 0
    first_base = jnp.where(first, x, y).astype(jnp.float32)
    second_base = jnp.where(first, y, x).astype(jnp.float32)
    outer = outer + first_base
    outer = jnp.where(outer >= 4.0, outer - 4.0, outer)
    inner = inner + second_base
    inner = jnp.where(inner >= 4.0, inner - 4.0, inner)
    last = last + z.astype(jnp.float32)
    last = jnp.where(last >= 2.0, last - 2.0, last)
    outer_stride = jnp.where(first, 8, 1).astype(jnp.float32)
    inner_stride = jnp.where(first, 1, 8).astype(jnp.float32)
    source = (outer * outer_stride + inner * inner_stride + last * 4.0) * share + rest
    unit = lax.broadcasted_iota(jnp.int32, (rows, hidden_units), 1).astype(jnp.float32)
    pick = jnp.where(source == unit, 1.0, 0.0).astype(jnp.bfloat16)
    by_sender = jnp.concatenate(
        [
            hidden_ref[local, pl.ds(jnp.bitwise_xor(own, m) * capacity, capacity), :]
            for m in range(4)
        ],
        axis=0,
    )
    out_ref[0] = lax.dot_general(
        pick, by_sender, (((1,), (1,)), ((), ())), preferred_element_type=jnp.float32
    ).astype(jnp.bfloat16)


def prepare(place, hidden):
    local_count, slots, units = hidden.shape
    return pl.pallas_call(
        prepare_body,
        grid_spec=pltpu.PrefetchScalarGridSpec(
            num_scalar_prefetch=1,
            grid=(local_count, 4),
            in_specs=[pl.BlockSpec(memory_space=pltpu.HBM)],
            out_specs=pl.BlockSpec((1, units // 4, slots), lambda e, b, s: (e, b, 0)),
            scratch_shapes=[
                pltpu.VMEM(hidden.shape, hidden.dtype),
                pltpu.SemaphoreType.DMA((local_count,)),
            ],
        ),
        out_shape=jax.ShapeDtypeStruct((local_count, units, slots), jnp.bfloat16),
        compiler_params=pltpu.CompilerParams(vmem_limit_bytes=20 * 2**20),
        name="prepare",
    )(place, hidden)


def matmul_body(ring, hidden_ref, r0, r1, r2, r3, *out_refs):
    rhs = jnp.concatenate([r[0] for r in (r0, r1, r2, r3)], axis=0)
    product = jnp.dot(hidden_ref[0], rhs, preferred_element_type=jnp.float32)
    half = product.shape[0] // 2
    each = len(out_refs) // 2
    for local in range(2):
        outs = out_refs[each * local : each * (local + 1)]
        for j in range(4):

            @pl.when(pl.program_id(0) == 4 * local + j)
            def store(j=j, outs=outs):
                if ring and j == 2:
                    outs[3][...] = product[:half].astype(jnp.bfloat16)
                    outs[4][...] = product[half:].astype(jnp.bfloat16)
                else:
                    out = outs[2 if ring and j == 3 else j]
                    out[...] = product.astype(out.dtype)


def partials(hidden, near, far, offset, ring):
    capacity, part = far[0].shape[1:]
    rows, slots = hidden.shape[1] // 4, hidden.shape[2]
    wide = jax.ShapeDtypeStruct((rows, part), jnp.float32)
    if ring:
        shapes = [wide] * 3 + [jax.ShapeDtypeStruct((rows // 2, part), jnp.bfloat16)] * 2
    else:
        shapes = [wide] + [jax.ShapeDtypeStruct((rows, part), jnp.bfloat16)] * 3
    near_spec = pl.BlockSpec(
        (pl.Element(1), pl.Element(capacity), pl.Element(part)), lambda i: (i // 4, 0, offset)
    )
    far_spec = pl.BlockSpec((1, capacity, part), lambda i: (i // 4, 0, 0))
    outs = pl.pallas_call(
        functools.partial(matmul_body, ring),
        grid=(8,),
        in_specs=[
            pl.BlockSpec((1, rows, slots), lambda i: (i // 4, i % 4, 0)),
            near_spec,
            near_spec,
            far_spec,
            far_spec,
        ],
        out_specs=[pl.BlockSpec(s.shape, lambda i: (0, 0)) for s in shapes * 2],
        out_shape=shapes * 2,
        compiler_params=pltpu.CompilerParams(vmem_limit_bytes=NARROW),
    )(hidden, *near, *far)
    return outs[: len(shapes)], outs[len(shapes) :]


def to_half(total):
    return (total * 0.03125).astype(jnp.float16)


def from_half(block):
    return block.astype(jnp.float32) * 32.0


def ring_sum(own, ahead, behind, low, high, along):
    half = low.shape[0]
    high = send(high, along[1])
    low = send(low, along[3])
    ahead = jnp.concatenate([ahead[:half], ahead[half:] + high.astype(jnp.float32)])
    behind = jnp.concatenate([behind[:half] + low.astype(jnp.float32), behind[half:]])
    ahead, behind = to_half(ahead), to_half(behind)
    ahead = send(ahead, along[1])
    behind = send(behind, along[3])
    return own + from_half(ahead) + from_half(behind)


def quarters(total):
    rows = total.shape[0] // 4
    pieces = [total[j * rows : (j + 1) * rows] for j in range(4)]
    return pieces[0], [to_half(piece) for piece in pieces[1:]]


def direct_sum(own, sends, along):
    got = []
    for j, block in zip((1, 2, 3), sends):
        got.append(send(block, along[j]))
    for block in got:
        own = own + (from_half(block) if block.dtype == jnp.float16 else block.astype(jnp.float32))
    return own


def step(cotangent, route_ids, route_weights, hidden, master, first_moment, second_moment):
    groups = lax.axis_size("expert")
    capacity = hidden.shape[1] // groups
    dp = lax.axis_index("dp").astype(jnp.int32)
    own = lax.axis_index("expert").astype(jnp.int32)
    place = jnp.stack([dp // 8, dp % 4, dp // 4 % 2, own])
    ids, weights = route_ids.T, route_weights.T
    gradients, received = [], []
    start = 0
    for group, widths in enumerate(GROUPS):
        if group == 1:
            place, _ = lax.optimization_barrier((place, far[0]))
            turned = prepare(place, hidden)
            own, turned = lax.optimization_barrier((own, turned))
        rows, far, farther = dispatch(
            own[None], ids, weights, cotangent, widths, start, group == 1, capacity
        )
        for index, width in enumerate(widths):
            one = send(far[index], TO_EXPERT[2])
            two = send(farther[index], TO_EXPERT[3])
            received.append(((one, two), start))
            start += width
    near = (rows[0], send(rows[1], TO_EXPERT[1]))
    totals = ([], [])
    for chunk, (far, offset) in enumerate(received):
        blocks = partials(turned, near, far, offset, RINGS[chunk])
        for local, along in enumerate((ALONG_X, ALONG_Y)):
            (own_block, *sends) = blocks[local]
            if RINGS[chunk]:
                total = ring_sum(own_block, *sends, along)
            else:
                total = direct_sum(own_block, sends, along)
            totals[local].append(total)
    for members in WAVES:
        halves = []
        for local, along in enumerate((ALONG_Y, ALONG_X)):
            total = jnp.concatenate([totals[local][c] for c in members], axis=1)
            own_block, sends = quarters(total)
            halves.append(direct_sum(own_block, sends, along))
        share = halves[0].shape[0] // 2
        away = jnp.stack([to_half(part[share:]) for part in halves])
        other = send(away, PAIR_Z)
        both = jnp.stack([part[:share] for part in halves]) + from_half(other)
        gradients.append(with_layout_constraint(both.transpose(1, 0, 2), ROW_MAJOR))
    summed = jnp.concatenate(gradients, axis=2)
    gradient = summed / jnp.sqrt(jnp.float32(groups * capacity))
    new_first = beta_one * first_moment + (1.0 - beta_one) * gradient
    new_second = beta_two * second_moment + (1.0 - beta_two) * gradient * gradient
    corrected_first = new_first / (1.0 - beta_one**step_count)
    corrected_second = new_second / (1.0 - beta_two**step_count)
    update = corrected_first / (jnp.sqrt(corrected_second) + epsilon) + decay_rate * master
    new_master = master - learning_rate * update
    return (new_master, new_first, new_second)


def solution(mesh):
    placed = (
        P(("dp", "expert"), None),
        P(("dp", "expert"), None),
        P(("dp", "expert"), None),
        P("expert", "dp", None),
        P("dp", "expert", None),
        P("dp", "expert", None),
        P("dp", "expert", None),
    )
    return jax.shard_map(
        step,
        mesh=mesh,
        in_specs=placed,
        out_specs=(P("dp", "expert", None), P("dp", "expert", None), P("dp", "expert", None)),
        check_vma=False,
    )
```
